128 devices in a mesh: dp: 32 (over z, y_hi, x), comp: 4 (over y_lo, core).
Axes of the slice: x: 4, y: 4 (y_hi: 2, y_lo: 2; y = y_hi * 2 + y_lo), z: 4, core: 2. Of those that a mesh axis runs over, the one named last changes fastest.
Arguments:
- points: float32 [4096, 1024], P('dp'), may hold values from -4.25 to 4.25
- centres: float32 [4096, 1024], P('comp'), may hold values from -1 to 1
- variances: float32 [4096, 1024], P('comp'), may hold values from 0.15 to 2
- mix_logits: float32 [4096], P('comp'), may hold values from -2 to 2
Outputs:
- new_centres: float32 [4096, 1024], P('comp')
- new_variances: float32 [4096, 1024], P('comp')
- log_weights: float32 [4096], P('comp')
- log_likelihood: float32 [4096], P('dp')
The draws below stay inside these ranges and needn't reach their ends.
All inputs are finite; a program needn't handle non-finite values.
Results may differ from the reference program's by a relative error of at most 0.0014.
Values sent between devices are 32-bit elements; how exact they have to be, the bound alone decides.
No kernel may reach another device: no remote copies, remote signals or barrier semaphores. Data moves between devices by JAX's collectives and lax.ppermute only.
A program may use at most 128 MiB of HBM per device.

```python
import math
import jax
import jax.numpy as jnp
from jax import lax

D = 1024
ITERS = 2
POINTS = 4096
K = 4096


def draw_points(key, part):
    inner = jax.random.fold_in(key, 101)
    values = 0.7071 * jax.random.truncated_normal(inner, -6.0, 6.0, (POINTS, D), jnp.float32)
    return values


def draw_centres(key, part):
    base_key, jitter_key = jax.random.split(jax.random.fold_in(key, 211))
    spread = 0.64 / math.sqrt(D)
    base = 0.2 * jax.random.truncated_normal(base_key, -3.0, 3.0, (1, D), jnp.float32)
    jitter = spread * jax.random.truncated_normal(jitter_key, -4.0, 4.0, (K, D), jnp.float32)
    return base + jitter


def draw_variances(key, part):
    base_key, jitter_key = jax.random.split(jax.random.fold_in(key, 307))
    spread = 1.8 / math.sqrt(D)
    low, high = (0.3, 1.0)
    base = jnp.exp(jax.random.uniform(base_key, (1, D), jnp.float32, math.log(low), math.log(high)))
    jitter = jax.random.uniform(jitter_key, (K, D), jnp.float32, -1.7320508, 1.7320508)
    return base * jnp.exp(spread * jitter)


def levels(stream_key, dims, shards, smallest, largest):
    def one(position, blocks):
        heights = jax.random.uniform(jax.random.fold_in(jax.random.fold_in(stream_key, 6), position), (blocks,), jnp.float32, smallest / len(shards), largest / len(shards))
        return jnp.repeat(jnp.exp(heights), dims[position] // blocks).reshape((-1,) + (1,) * (len(dims) - position - 1))

    level = one(*shards[0])
    for cut in shards[1:]:
        level = level * one(*cut)
    return level


def setup_inputs(seed: int = 0) -> dict:
    splits = jax.random.split(jax.random.key(seed), 5)
    return {
        "points": draw_points(jax.random.fold_in(splits[4], 71), 0),
        "centres": draw_centres(jax.random.fold_in(splits[4], 71), 0),
        "variances": draw_variances(jax.random.fold_in(splits[4], 71), 0),
        "mix_logits": jnp.clip(jax.random.uniform(splits[3], (K,), jnp.float32, -2.0, 2.0) * levels(splits[3], (K,), ((0, 4),), -0.4, 0.0), -2.0, 2.0),
    }


LOG_TWO_PI = math.log(2.0 * math.pi)


def contract_rows(left, right):
    return lax.dot_general(left, right, (((1,), (1,)), ((), ())), precision=lax.Precision.HIGHEST, preferred_element_type=jnp.float32)


def contract_points(shares, values):
    return lax.dot_general(shares, values, (((0,), (0,)), ((), ())), precision=lax.Precision.HIGHEST, preferred_element_type=jnp.float32)


def expect(points, squares, centres, variances, mix_logits):
    inverse = 1.0 / variances
    scaled = centres * inverse
    offset = jnp.sum(centres * scaled, 1) + jnp.sum(jnp.log(variances), 1) + points.shape[1] * LOG_TWO_PI
    quadratic = contract_rows(squares, inverse) - 2.0 * contract_rows(points, scaled)
    return mix_logits[None, :] - 0.5 * (quadratic + offset[None, :])


def update(counts, first, second, denominator):
    plus_one = (counts + 1.0)[:, None]
    centre_new = first / plus_one
    spread_new = (second - 2.0 * centre_new * first + plus_one * centre_new * centre_new + 1.0) / (counts + 2.0)[:, None]
    logit_new = jnp.log((counts + 1.0) / denominator)
    return centre_new, spread_new, logit_new


def reference(points, centres, variances, mix_logits):
    squares = points * points
    denominator = jnp.float32(points.shape[0] + centres.shape[0])
    log_norm = jnp.zeros((points.shape[0],), jnp.float32)
    for iteration in range(ITERS):
        density = expect(points, squares, centres, variances, mix_logits)
        highest = jnp.max(density, 1)
        summed = jnp.sum(jnp.exp(density - highest[:, None]), 1)
        log_norm = highest + jnp.log(summed)
        shares = jnp.exp(density - log_norm[:, None])
        counts = jnp.sum(shares, 0)
        first = contract_points(shares, points)
        second = contract_points(shares, squares)
        centres, variances, mix_logits = update(counts, first, second, denominator)
    return centres, variances, mix_logits, log_norm
```

```python
import math

import jax
import jax.numpy as jnp
from jax import lax
from jax.sharding import Mesh
from jax.sharding import PartitionSpec as P

ITERS = 2
LOG_TWO_PI = math.log(2.0 * math.pi)
POINT_AXES = ("z", "yh", "x")
COMP_AXES = ("yl", "c")
PLANE = ("z", "x")
NORM_AXES = ("z", "x", "yl")


def shift(value, axis, step):
    n = lax.axis_size(axis)
    return lax.ppermute(value, axis, [(i, (i + step) % n) for i in range(n)])


def contract(left, right, dims):
    return lax.dot_general(
        left,
        right,
        ((dims, dims), ((), ())),
        precision=lax.Precision.HIGHEST,
        preferred_element_type=jnp.float32,
    )


def put(into, piece, at, dim):
    return lax.dynamic_update_slice_in_dim(into, jnp.expand_dims(piece, dim), at, dim)


def ring_direct(piece, axis, dim):
    n = lax.axis_size(axis)
    me = lax.axis_index(axis)
    got = {0: piece}
    for step in (1, n - 1, *range(2, n - 1)):
        got[step] = shift(piece, axis, step)
    shape = list(piece.shape)
    shape.insert(dim, n)
    out = jnp.zeros(shape, piece.dtype)
    for step, part in got.items():
        out = put(out, part, (me - step) % n, dim)
    return out


def ring_forward(block, axis, dim):
    n = lax.axis_size(axis)
    me = lax.axis_index(axis)
    half = block.shape[0] // 2
    back = shift(block, axis, 1)
    ahead = shift(block, axis, n - 1)
    far_first = shift(back[:half], axis, 1)
    far_last = shift(ahead[half:], axis, n - 1)
    far = jnp.concatenate([far_first, far_last], 0)
    shape = list(block.shape)
    shape.insert(dim, n)
    out = jnp.zeros(shape, block.dtype)
    for step, part in ((0, block), (1, back), (n - 1, ahead), (2, far)):
        out = put(out, part, (me - step) % n, dim)
    return out


def plane_gather(first, second):
    a = ring_direct(first, "x", 0)
    b = ring_direct(second, "z", 0)
    a = ring_forward(a, "z", 0)
    b = ring_forward(b, "x", 1)
    return a, b


def plane_gather_small(piece):
    return ring_direct(ring_direct(piece, "x", 0), "z", 0)


def density_of(points, squares, centres, variances, logits):
    inverse = 1.0 / variances
    scaled = centres * inverse
    offset = (
        jnp.sum(centres * scaled, 1) + jnp.sum(jnp.log(variances), 1) + points.shape[1] * LOG_TWO_PI
    )
    quadratic = contract(squares, inverse, (1,)) - 2.0 * contract(points, scaled, (1,))
    return logits[None, :] - 0.5 * (quadratic + offset[None, :])


def everyones(piece, axes):
    copies = jnp.broadcast_to(piece, (lax.axis_size(axes), *piece.shape))
    return lax.all_to_all(copies, axes, split_axis=0, concat_axis=0, tiled=True)


def log_norm_of(density):
    highest = jnp.max(density, 1)
    summed = jnp.sum(jnp.exp(density - highest[:, None]), 1)
    pairs = everyones(jnp.stack([highest, summed]).reshape(2, 8, -1), NORM_AXES)
    top = jnp.max(pairs[:, 0], 0)
    total = jnp.sum(pairs[:, 1] * jnp.exp(pairs[:, 0] - top), 0)
    return (top + jnp.log(total)).reshape(-1)


def on_device(points, centres, variances, logits):
    rows = points.shape[0]
    comp_rows = centres.shape[0]
    plane = lax.axis_size(PLANE)
    core = lax.axis_index("c")
    spot = lax.axis_index(PLANE)
    denominator = jnp.float32(
        rows * lax.axis_size(POINT_AXES) + comp_rows * lax.axis_size(COMP_AXES)
    )

    half = rows // 2
    mine = lax.dynamic_slice_in_dim(points, core * half, half, 0)
    part_a, part_b = plane_gather(mine[: half // 2], mine[half // 2 :])
    width = points.shape[1]
    points = jnp.concatenate([part_a.reshape(-1, width), part_b.reshape(-1, width)], 0)
    squares = points * points

    share = comp_rows // plane
    centre = lax.dynamic_slice_in_dim(centres, spot * share, share, 0)
    spread = lax.dynamic_slice_in_dim(variances, spot * share, share, 0)
    logit = lax.dynamic_slice_in_dim(logits, spot * share, share, 0)

    for iteration in range(ITERS):
        both_c, both_v, both_l = (
            jnp.concatenate([own, shift(own, "c", 1)], 0) for own in (centre, spread, logit)
        )
        density = density_of(points, squares, both_c, both_v, both_l)
        log_norm = log_norm_of(density)
        shares = jnp.exp(density - log_norm[:, None])
        parts = (
            jnp.sum(shares, 0),
            contract(shares, points, (0,)),
            contract(shares, squares, (0,)),
        )
        parts = [p[:share] + shift(p[share:], "c", 1) for p in parts]
        counts, first, second = (p + shift(p, "yh", 1) for p in parts)
        plus_one = (counts + 1.0)[:, None]
        centre = first / plus_one
        spread = (second - 2.0 * centre * first + plus_one * centre * centre + 1.0) / (
            counts + 2.0
        )[:, None]
        logit = jnp.log((counts + 1.0) / denominator)

    log_weights = plane_gather_small(logit).reshape(-1)
    new_centres, new_variances = plane_gather(centre, spread)

    by_piece = log_norm.reshape(2, plane, half // 2)
    own = lax.dynamic_index_in_dim(by_piece, spot, 1, keepdims=False).reshape(-1)
    other = shift(own, "c", 1)
    likelihood = jnp.where(
        core == 0, jnp.concatenate([own, other]), jnp.concatenate([other, own])
    )
    return (
        new_centres.reshape(comp_rows, width),
        new_variances.reshape(comp_rows, width),
        log_weights,
        likelihood,
    )


def solution(mesh):
    finer = Mesh(mesh.devices.reshape(4, 2, 4, 2, 2), ("z", "yh", "x", "yl", "c"))
    in_specs = (P(POINT_AXES, None), P(COMP_AXES, None), P(COMP_AXES, None), P(COMP_AXES))
    out_specs = (P(COMP_AXES, None), P(COMP_AXES, None), P(COMP_AXES), P(POINT_AXES))
    return jax.shard_map(
        on_device, mesh=finer, in_specs=in_specs, out_specs=out_specs, check_vma=False
    )
```
